32 devices in a mesh: row: 8 (over z, x), col: 4 (over y, core).
Axes of the slice: x: 2, y: 2, z: 4, core: 2. Of those that a mesh axis runs over, the one named last changes fastest.
Arguments:
- normal_matrix: float32 [9216, 9216], P('row', 'col'), may hold values from -1 to 6, as said below
- right_side: float32 [9216, 64], P('col'), may hold values from -6 to 6
- tile_inverse: float32 [72, 128, 128], P('col'), may hold values from -1 to 3.5, as said below
- order_ids: int32 [9216], P('col'), may hold values from 0 to 96, never falling along the last dimension, each value on 1 to 194 neighbouring positions
Outputs:
- solution: float32 [9216, 64], P('col')
- residual: float32 [9216, 64], P('col')
The draws below stay inside these ranges and needn't reach their ends.
Inputs may be any that keep to these rules, and one draw needn't show every extreme that they name: `normal_matrix`: symmetric and positive definite. `tile_inverse`: each tile symmetric, every principal submatrix of it positive definite. `order_ids`: never falling along the coefficients; each order holds 1 to 194 coefficients.
All inputs are finite; a program needn't handle non-finite values.
Results may differ from the reference program's by a relative error of at most 0.0003.
Values sent between devices are 32-bit elements; how exact they have to be, the bound alone decides.
A program may use at most 64 MiB of HBM per device.

```python
import math
import jax
import jax.numpy as jnp
import numpy as np
from jax import lax

NUM = 9216
ORDERS = 97
ORDER_MOST = 194
BLK = 128
NRHS = 64
ITERS = 2


def draw_normal_matrix(key, part):
    first, second = jax.random.split(jax.random.fold_in(key, 11))
    raw = jax.random.normal(first, (NUM, NUM), jnp.float32)
    symmetric = (raw + raw.T) * (0.5 / math.sqrt(NUM))
    diagonal = jax.random.uniform(second, (NUM,), jnp.float32, 2.0, 4.0)
    return symmetric + jnp.diag(diagonal)


def draw_tile_inverse(key, part):
    first, second = jax.random.split(jax.random.fold_in(key, 23))
    raw = jax.random.normal(first, (NUM // BLK, BLK, BLK), jnp.float32)
    symmetric = (raw + jnp.swapaxes(raw, 1, 2)) * (0.3 / math.sqrt(BLK))
    diagonal = jax.random.uniform(second, (NUM // BLK, BLK), jnp.float32, 1.0, 3.0)
    eye = jnp.eye(BLK, dtype=jnp.float32)
    return symmetric + diagonal[:, :, None] * eye[None, :, :]


def block_levels(rng, dims, cuts, least, top_value):
    loudness = 1.0
    for dim, blocks in cuts:
        steps = jax.random.uniform(jax.random.fold_in(jax.random.fold_in(rng, 6), dim), (blocks,), jnp.float32, least / len(cuts), top_value / len(cuts))
        loudness = loudness * jnp.repeat(jnp.exp(steps), dims[dim] // blocks).reshape((-1,) + (1,) * (len(dims) - 1 - dim))
    return loudness


def profile(count, total, limit, lean):
    loads = [(1 << 20) // math.isqrt(standing ** lean) + 1 for standing in range(2, count + 1)]
    surplus, given = total - limit - (count - 1), [1] * (count - 1)
    while surplus > 0:
        free = [i for i in range(count - 1) if given[i] < limit]
        mass, remaining = sum([loads[i] for i in free]), surplus
        for i in free:
            extra = min(limit - given[i], max(1, remaining * loads[i] // mass), surplus)
            given[i] = given[i] + extra
            surplus = surplus - extra
    return np.array([limit] + given)


def ragged(own_key, number_of, total, bound, lean):
    if number_of == 2:
        one = jax.random.randint(own_key, (), max(1, total - bound), min(bound, total - 1) + 1)
        return jnp.stack([one, total - one])
    sizes = jnp.asarray(profile(number_of, total, bound, lean), jnp.int32)
    pairs = (number_of - 1) // 2
    giver, sink = sizes[1:1 + 2 * pairs:2], sizes[2:2 + 2 * pairs:2]
    margin = jnp.minimum(giver - 1, bound - sink)
    passed = jax.random.randint(jax.random.fold_in(own_key, 1), (pairs,), 0, 1 << 20) % (margin + 1)
    sizes = sizes.at[1:1 + 2 * pairs:2].set(giver - passed).at[2:2 + 2 * pairs:2].set(sink + passed)
    return sizes[jax.random.permutation(jax.random.fold_in(own_key, 2), number_of)]


def centred(stream_key, shape, deviation, reach, shards=(), kind=jnp.bfloat16):
    values = deviation * jax.random.normal(stream_key, shape, jnp.float32)
    if shards:
        values = values * block_levels(stream_key, shape, shards, -0.22, 0.18)
    return jnp.clip(values, -reach, reach).astype(kind)


def setup_inputs(seed: int = 0) -> dict:
    keys = jax.random.split(jax.random.key(seed), 5)
    normal_matrix = draw_normal_matrix(jax.random.fold_in(keys[4], 71), 0)
    right_side = centred(keys[1], (NUM, NRHS), 1.0, 6.0, ((0, 4),), jnp.float32)
    tile_inverse = draw_tile_inverse(jax.random.fold_in(keys[4], 71), 0)
    order_ids = jnp.searchsorted(jnp.cumsum(ragged(keys[3], ORDERS, NUM, ORDER_MOST, 0)), jnp.arange(NUM), side="right").astype(jnp.int32)
    return {"normal_matrix": normal_matrix, "right_side": right_side, "tile_inverse": tile_inverse, "order_ids": order_ids}


def apply_precond(tile_inverse, order_ids, vector):
    count = tile_inverse.shape[0]
    width = tile_inverse.shape[1]
    order_tile = order_ids.reshape(count, width)
    same_order = order_tile[:, :, None] == order_tile[:, None, :]
    masked = jnp.where(same_order, tile_inverse, jnp.float32(0.0))
    pieces = vector.reshape(count, width, vector.shape[1])
    result = jnp.einsum("tij,tjk->tik", masked, pieces, precision=lax.Precision.HIGHEST)
    return result.reshape(vector.shape)


def reference(normal_matrix, right_side, tile_inverse, order_ids):
    def apply_matrix(vector):
        return jnp.dot(normal_matrix, vector, precision=lax.Precision.HIGHEST, preferred_element_type=jnp.float32)

    solution = jnp.zeros_like(right_side)
    residual = right_side
    precond_res = apply_precond(tile_inverse, order_ids, residual)
    image_res = apply_matrix(precond_res)
    image_dir = jnp.zeros_like(right_side)
    precond_dir = jnp.zeros_like(right_side)
    residual_dir = jnp.zeros_like(right_side)
    direction = jnp.zeros_like(right_side)
    gamma_prev = jnp.ones((right_side.shape[1],), jnp.float32)
    alpha_prev = jnp.ones((right_side.shape[1],), jnp.float32)
    for iteration in range(ITERS):
        gamma_now = jnp.sum(residual * precond_res, axis=0)
        delta_now = jnp.sum(image_res * precond_res, axis=0)
        precond_img = apply_precond(tile_inverse, order_ids, image_res)
        image_img = apply_matrix(precond_img)
        if iteration == 0:
            beta_ratio = jnp.zeros_like(gamma_now)
            step_size = gamma_now / delta_now
        else:
            beta_ratio = gamma_now / gamma_prev
            step_size = gamma_now / (delta_now - beta_ratio * gamma_now / alpha_prev)
        image_dir = image_img + beta_ratio * image_dir
        precond_dir = precond_img + beta_ratio * precond_dir
        residual_dir = image_res + beta_ratio * residual_dir
        direction = precond_res + beta_ratio * direction
        solution = solution + step_size * direction
        residual = residual - step_size * residual_dir
        precond_res = precond_res - step_size * precond_dir
        image_res = image_res - step_size * image_dir
        gamma_prev = gamma_now
        alpha_prev = step_size
    return solution, residual
```

```python
import functools

import jax
import jax.numpy as jnp
from jax import lax
from jax.experimental import pallas as pl
from jax.experimental.pallas import tpu as pltpu
from jax.sharding import PartitionSpec as P

ITERS = 2
MESH = pl.DeviceIdType.MESH


def masked_tiles(tile_inverse, order_ids):
    count = tile_inverse.shape[0]
    width = tile_inverse.shape[1]
    order_tile = order_ids.reshape(count, width)
    same_order = order_tile[:, :, None] == order_tile[:, None, :]
    return jnp.where(same_order, tile_inverse, jnp.float32(0.0))


def apply_precond(tile_inverse, order_ids, vector):
    count = tile_inverse.shape[0]
    width = tile_inverse.shape[1]
    masked = masked_tiles(tile_inverse, order_ids)
    pieces = vector.reshape(count, width, vector.shape[1])
    result = jnp.einsum("tij,tjk->tik", masked, pieces, precision=lax.Precision.HIGHEST)
    return result.reshape(vector.shape)


def plain_body(normal_matrix, right_side, tile_inverse, order_ids):
    block_rows = normal_matrix.shape[0]

    def apply_matrix(vector):
        first_row = lax.axis_index("row") * block_rows
        gathered = lax.all_gather(vector, "col", axis=0, tiled=True)
        row_piece = lax.dynamic_slice_in_dim(gathered, first_row, block_rows, 0)
        partial_value = lax.dot_general(
            normal_matrix,
            row_piece,
            (((0,), (0,)), ((), ())),
            precision=lax.Precision.HIGHEST,
            preferred_element_type=jnp.float32,
        )
        return lax.psum(partial_value, "row")

    solution = jnp.zeros_like(right_side)
    residual = right_side
    precond_res = apply_precond(tile_inverse, order_ids, residual)
    image_res = apply_matrix(precond_res)
    image_dir = jnp.zeros_like(right_side)
    precond_dir = jnp.zeros_like(right_side)
    residual_dir = jnp.zeros_like(right_side)
    direction = jnp.zeros_like(right_side)
    gamma_prev = jnp.ones((right_side.shape[1],), jnp.float32)
    alpha_prev = jnp.ones((right_side.shape[1],), jnp.float32)
    for iteration in range(ITERS):
        gamma_now, delta_now = lax.psum(
            (jnp.sum(residual * precond_res, axis=0), jnp.sum(image_res * precond_res, axis=0)),
            "col",
        )
        precond_img = apply_precond(tile_inverse, order_ids, image_res)
        image_img = apply_matrix(precond_img)
        if iteration == 0:
            beta_ratio = jnp.zeros_like(gamma_now)
            step_size = gamma_now / delta_now
        else:
            beta_ratio = gamma_now / gamma_prev
            step_size = gamma_now / (delta_now - beta_ratio * gamma_now / alpha_prev)
        image_dir = image_img + beta_ratio * image_dir
        precond_dir = precond_img + beta_ratio * precond_dir
        residual_dir = image_res + beta_ratio * residual_dir
        direction = precond_res + beta_ratio * direction
        solution = solution + step_size * direction
        residual = residual - step_size * residual_dir
        precond_res = precond_res - step_size * precond_dir
        image_res = image_res - step_size * image_dir
        gamma_prev = gamma_now
        alpha_prev = step_size
    return (solution, residual)


def split(value):
    high = value.astype(jnp.bfloat16)
    low = (value - high.astype(jnp.float32)).astype(jnp.bfloat16)
    return jnp.concatenate([high, low], axis=0)


def times_transposed(left, right):
    return lax.dot_general(
        left, right, (((1,), (1,)), ((), ())), preferred_element_type=jnp.float32
    )


def fold(product, rows, columns):
    upper = product[:rows, :columns] + product[rows:, :columns]
    lower = product[:rows, columns:] + product[rows:, columns:]
    return upper + lower


def kernel(
    row_count, group, chunks, width,
    a_ref, tile_ref, b_ref,
    sol_ref, res_ref,
    a_buf, a_split, tile_split, v_split, u_buf, m_buf,
    part, near, half, far, full, image,
    dot_own, dot_in,
    a_sem, near_sem, far_sem, full_sem, line_recv, line_send, side_recv, side_send, dot_send, dot_recv,
):
    my_row, my_col = lax.axis_index("row"), lax.axis_index("col")
    depth = row_count // group
    place, lane = my_row // group, lax.rem(my_row, group)
    core = lax.rem(my_col, 2)
    partner = my_col + 1 - 2 * core
    across = lax.rem(my_col + 2, 4)
    nrhs, block_cols = b_ref.shape
    block_rows = a_ref.shape[0]
    hh = nrhs // 2
    tiles = block_cols // width
    steps = block_rows // width
    piece = block_rows // chunks

    def fetch(i):
        rows = pl.ds(pl.multiple_of(i * width, width), width)
        return pltpu.make_async_copy(a_ref.at[rows], a_buf.at[i], a_sem.at[i])

    @pl.loop(0, steps)
    def _(i):
        fetch(i).start()

    barrier = pltpu.get_barrier_semaphore()
    for shift in range(1, 4):
        pl.semaphore_signal(
            barrier, inc=1, device_id=(my_row, lax.rem(my_col + shift, 4)), device_id_type=MESH
        )
    for shift in range(1, group):
        side = place * group + lax.rem(lane + shift, group)
        pl.semaphore_signal(barrier, inc=1, device_id=(side, my_col), device_id_type=MESH)

    @pl.when(place > 0)
    def _():
        pl.semaphore_signal(barrier, inc=1, device_id=(my_row - group, my_col), device_id_type=MESH)

    @pl.when(place < depth - 1)
    def _():
        pl.semaphore_signal(barrier, inc=1, device_id=(my_row + group, my_col), device_id_type=MESH)

    def tile_lanes(t):
        return pl.ds(pl.multiple_of(t * width, width), width)

    def precondition(source, target):
        @pl.loop(0, tiles)
        def _(t):
            lanes = tile_lanes(t)
            value = fold(times_transposed(split(source[:, lanes]), tile_split[t]), nrhs, width)
            target[:, lanes] = value
            v_split[:, lanes] = split(value)

    @pl.loop(0, tiles)
    def _(t):
        tile_split[t] = split(tile_ref[t])

    precondition(b_ref, u_buf)

    def reduce_and_spread(turn):
        def swap(source, target, sem, column):
            return pltpu.make_async_remote_copy(
                src_ref=source, dst_ref=target, send_sem=sem.at[turn, 0], recv_sem=sem.at[turn, 1],
                device_id=(my_row, column), device_id_type=MESH,
            )

        mine = pl.ds(pl.multiple_of(core * hh, hh), hh)
        other = pl.ds(pl.multiple_of((1 - core) * hh, hh), hh)
        first = swap(part.at[turn, other], near.at[turn], near_sem, partner)
        first.start()
        first.wait()
        half[turn] = part[turn, mine] + near[turn]
        second = swap(half.at[turn], far.at[turn], far_sem, across)
        second.start()
        second.wait()
        full[turn, mine] = half[turn] + far[turn]
        third = swap(full.at[turn, mine], full.at[turn, mine], full_sem, partner)
        third.start()
        third.wait()

        @pl.when(place == my_col)
        def _():
            start = pl.multiple_of(lane * block_rows, width)
            image[turn, :, pl.ds(start, block_rows)] = full[turn]

        def lanes_of(owner, q):
            start = pl.multiple_of(owner * block_rows + q * piece, width)
            return image.at[turn, :, pl.ds(start, piece)]

        def along(q, way, target_row):
            return pltpu.make_async_remote_copy(
                src_ref=lanes_of(lane, q), dst_ref=lanes_of(lane, q),
                send_sem=line_send.at[turn, way, q], recv_sem=line_recv.at[turn, q],
                device_id=(target_row, my_col), device_id_type=MESH,
            )

        def sideways(q, shift):
            side = place * group + lax.rem(lane + shift, group)
            return pltpu.make_async_remote_copy(
                src_ref=lanes_of(lane, q), dst_ref=lanes_of(lane, q),
                send_sem=side_send.at[turn, shift - 1, q], recv_sem=side_recv.at[turn, shift - 1, q],
                device_id=(side, my_col), device_id_type=MESH,
            )

        def arrived(q, shift):
            origin = lax.rem(lane + group - shift, group)
            return pltpu.make_async_remote_copy(
                src_ref=lanes_of(origin, q), dst_ref=lanes_of(origin, q),
                send_sem=side_send.at[turn, shift - 1, q], recv_sem=side_recv.at[turn, shift - 1, q],
                device_id=(place * group + origin, my_col), device_id_type=MESH,
            )

        goes_up = jnp.logical_and(place >= my_col, place < depth - 1)
        goes_down = jnp.logical_and(place <= my_col, place > 0)
        for q in range(chunks):
            @pl.when(place != my_col)
            def _():
                along(q, 0, my_row).wait_recv()

            @pl.when(goes_up)
            def _():
                along(q, 0, my_row + group).start()

            @pl.when(goes_down)
            def _():
                along(q, 1, my_row - group).start()

            for shift in range(1, group):
                sideways(q, shift).start()

        for q in range(chunks):
            for shift in range(1, group):
                arrived(q, shift).wait_recv()

        def finish():
            for q in range(chunks):
                @pl.when(goes_up)
                def _():
                    along(q, 0, my_row + group).wait_send()

                @pl.when(goes_down)
                def _():
                    along(q, 1, my_row - group).wait_send()

                for shift in range(1, group):
                    sideways(q, shift).wait_send()

        return finish

    def dots_copy(turn, shift):
        return pltpu.make_async_remote_copy(
            src_ref=dot_own.at[turn], dst_ref=dot_in.at[turn, shift - 1],
            send_sem=dot_send.at[turn, shift - 1], recv_sem=dot_recv.at[turn, shift - 1],
            device_id=(my_row, lax.rem(my_col + shift, 4)), device_id_type=MESH,
        )

    def pack(gamma, delta):
        place_of = lax.broadcasted_iota(jnp.int32, (nrhs, width), 1)
        gamma = jnp.sum(gamma, axis=1, keepdims=True)
        delta = jnp.sum(delta, axis=1, keepdims=True)
        return jnp.where(place_of == 0, gamma, jnp.where(place_of == 1, delta, 0.0))

    def unpack(turn):
        total = [dot_own[turn]] + [dot_in[turn, (3 - my_col_shift)] for my_col_shift in (1, 2, 3)]
        total = (total[0] + total[2]) + (total[1] + total[3])
        return total[:, 0:1], total[:, 1:2]

    @pl.loop(0, steps)
    def _(i):
        fetch(i).wait()
        parts = split(a_buf[i])
        a_split[i] = parts
        part[0, :, tile_lanes(i)] = fold(times_transposed(v_split[...], parts), nrhs, width)

    pl.semaphore_wait(
        barrier,
        3 + (group - 1) + jnp.where(place > 0, 1, 0) + jnp.where(place < depth - 1, 1, 0),
    )
    finish_first = reduce_and_spread(0)

    zeros = jnp.zeros((nrhs, width), jnp.float32)

    def first_dots(t, carry):
        lanes = tile_lanes(t)
        u = u_buf[:, lanes]
        return carry[0] + b_ref[:, lanes] * u, carry[1] + image[0, :, lanes] * u

    dot_own[0] = pack(*lax.fori_loop(0, tiles, first_dots, (zeros, zeros)))
    for shift in (2, 1, 3):
        dots_copy(0, shift).start()

    precondition(image.at[0], m_buf)

    @pl.loop(0, steps)
    def _(i):
        part[1, :, tile_lanes(i)] = fold(times_transposed(v_split[...], a_split[i]), nrhs, width)

    for shift in range(1, 4):
        dots_copy(0, shift).wait()
    finish_first()
    finish_second = reduce_and_spread(1)

    gamma0, delta0 = unpack(0)
    alpha0 = gamma0 / delta0

    def second_dots(t, carry):
        lanes = tile_lanes(t)
        res = b_ref[:, lanes] - alpha0 * image[0, :, lanes]
        pre = u_buf[:, lanes] - alpha0 * m_buf[:, lanes]
        img = image[0, :, lanes] - alpha0 * image[1, :, lanes]
        res_ref[:, lanes] = res
        m_buf[:, lanes] = pre
        return carry[0] + res * pre, carry[1] + img * pre

    dot_own[1] = pack(*lax.fori_loop(0, tiles, second_dots, (zeros, zeros)))
    for shift in (2, 1, 3):
        dots_copy(1, shift).start()
    for shift in range(1, 4):
        dots_copy(1, shift).wait()
    gamma1, delta1 = unpack(1)
    beta = gamma1 / gamma0
    alpha1 = gamma1 / (delta1 - beta * gamma1 / alpha0)

    @pl.loop(0, tiles)
    def _(t):
        lanes = tile_lanes(t)
        u = u_buf[:, lanes]
        w = image[0, :, lanes]
        img = w - alpha0 * image[1, :, lanes]
        sol_ref[:, lanes] = alpha0 * u + alpha1 * (m_buf[:, lanes] + beta * u)
        res_ref[:, lanes] = res_ref[:, lanes] - alpha1 * (img + beta * w)

    finish_second()


def fused_body(row_count, group, normal_matrix, right_side, tile_inverse, order_ids):
    block_rows, block_cols = normal_matrix.shape
    nrhs = right_side.shape[1]
    tiles, width = tile_inverse.shape[:2]
    steps = block_rows // width
    chunks = 3 if steps % 3 == 0 else 1
    f32, bf16 = jnp.float32, jnp.bfloat16
    out = jax.ShapeDtypeStruct((nrhs, block_cols), f32)
    dma = pltpu.SemaphoreType.DMA
    vmem = pl.BlockSpec(memory_space=pltpu.VMEM)
    sol, res = pl.pallas_call(
        functools.partial(kernel, row_count, group, chunks, width),
        out_shape=(out, out),
        in_specs=[pl.BlockSpec(memory_space=pl.ANY), vmem, vmem],
        out_specs=(vmem, vmem),
        scratch_shapes=[
            pltpu.VMEM((steps, width, block_cols), f32),
            pltpu.VMEM((steps, 2 * width, block_cols), bf16),
            pltpu.VMEM((tiles, 2 * width, width), bf16),
            pltpu.VMEM((2 * nrhs, block_cols), bf16),
            pltpu.VMEM((nrhs, block_cols), f32),
            pltpu.VMEM((nrhs, block_cols), f32),
            pltpu.VMEM((2, nrhs, block_rows), f32),
            pltpu.VMEM((2, nrhs // 2, block_rows), f32),
            pltpu.VMEM((2, nrhs // 2, block_rows), f32),
            pltpu.VMEM((2, nrhs // 2, block_rows), f32),
            pltpu.VMEM((2, nrhs, block_rows), f32),
            pltpu.VMEM((2, nrhs, block_cols), f32),
            pltpu.VMEM((2, nrhs, width), f32),
            pltpu.VMEM((2, 3, nrhs, width), f32),
            dma((steps,)),
            dma((2, 2)),
            dma((2, 2)),
            dma((2, 2)),
            dma((2, chunks)),
            dma((2, 2, chunks)),
            dma((2, group - 1, chunks)),
            dma((2, group - 1, chunks)),
            dma((2, 3)),
            dma((2, 3)),
        ],
        compiler_params=pltpu.CompilerParams(
            collective_id=0, has_side_effects=True, vmem_limit_bytes=60 * 1024 * 1024
        ),
    )(normal_matrix, masked_tiles(tile_inverse, order_ids), right_side.T)
    return sol.T, res.T


def body(row_count, col_count, normal_matrix, right_side, tile_inverse, order_ids):
    block_rows, block_cols = normal_matrix.shape
    width = tile_inverse.shape[1]
    group = block_cols // block_rows
    fits = (
        col_count == 4
        and group > 1
        and row_count == group * col_count
        and block_rows % width == 0
        and width % 128 == 0
        and right_side.shape[1] % 32 == 0
    )
    if fits:
        return fused_body(row_count, group, normal_matrix, right_side, tile_inverse, order_ids)
    return plain_body(normal_matrix, right_side, tile_inverse, order_ids)


def solution(mesh):
    return jax.shard_map(
        functools.partial(body, mesh.shape["row"], mesh.shape["col"]),
        mesh=mesh,
        in_specs=(P("row", "col"), P("col", None), P("col", None, None), P("col")),
        out_specs=(P("col", None), P("col", None)),
        check_vma=False,
    )
```

```python
import functools

import jax
import jax.numpy as jnp
from jax import lax
from jax.experimental import pallas as pl
from jax.experimental.pallas import tpu as pltpu
from jax.sharding import PartitionSpec as P

ITERS = 2
MESH = pl.DeviceIdType.MESH
CHUNKS = 9
LAGS = (0, 2, 6, 8)


def masked_tiles(tile_inverse, order_ids):
    count = tile_inverse.shape[0]
    width = tile_inverse.shape[1]
    order_tile = order_ids.reshape(count, width)
    same_order = order_tile[:, :, None] == order_tile[:, None, :]
    return jnp.where(same_order, tile_inverse, jnp.float32(0.0))


def apply_precond(tile_inverse, order_ids, vector):
    count = tile_inverse.shape[0]
    width = tile_inverse.shape[1]
    masked = masked_tiles(tile_inverse, order_ids)
    pieces = vector.reshape(count, width, vector.shape[1])
    result = jnp.einsum("tij,tjk->tik", masked, pieces, precision=lax.Precision.HIGHEST)
    return result.reshape(vector.shape)


def plain_body(normal_matrix, right_side, tile_inverse, order_ids):
    block_rows = normal_matrix.shape[0]

    def apply_matrix(vector):
        first_row = lax.axis_index("row") * block_rows
        gathered = lax.all_gather(vector, "col", axis=0, tiled=True)
        row_piece = lax.dynamic_slice_in_dim(gathered, first_row, block_rows, 0)
        partial_value = lax.dot_general(
            normal_matrix,
            row_piece,
            (((0,), (0,)), ((), ())),
            precision=lax.Precision.HIGHEST,
            preferred_element_type=jnp.float32,
        )
        return lax.psum(partial_value, "row")

    solution = jnp.zeros_like(right_side)
    residual = right_side
    precond_res = apply_precond(tile_inverse, order_ids, residual)
    image_res = apply_matrix(precond_res)
    image_dir = jnp.zeros_like(right_side)
    precond_dir = jnp.zeros_like(right_side)
    residual_dir = jnp.zeros_like(right_side)
    direction = jnp.zeros_like(right_side)
    gamma_prev = jnp.ones((right_side.shape[1],), jnp.float32)
    alpha_prev = jnp.ones((right_side.shape[1],), jnp.float32)
    for iteration in range(ITERS):
        gamma_now, delta_now = lax.psum(
            (jnp.sum(residual * precond_res, axis=0), jnp.sum(image_res * precond_res, axis=0)),
            "col",
        )
        precond_img = apply_precond(tile_inverse, order_ids, image_res)
        image_img = apply_matrix(precond_img)
        if iteration == 0:
            beta_ratio = jnp.zeros_like(gamma_now)
            step_size = gamma_now / delta_now
        else:
            beta_ratio = gamma_now / gamma_prev
            step_size = gamma_now / (delta_now - beta_ratio * gamma_now / alpha_prev)
        image_dir = image_img + beta_ratio * image_dir
        precond_dir = precond_img + beta_ratio * precond_dir
        residual_dir = image_res + beta_ratio * residual_dir
        direction = precond_res + beta_ratio * direction
        solution = solution + step_size * direction
        residual = residual - step_size * residual_dir
        precond_res = precond_res - step_size * precond_dir
        image_res = image_res - step_size * image_dir
        gamma_prev = gamma_now
        alpha_prev = step_size
    return (solution, residual)


def split(value):
    high = value.astype(jnp.bfloat16)
    low = (value - high.astype(jnp.float32)).astype(jnp.bfloat16)
    return jnp.concatenate([high, low], axis=0)


def times_transposed(left, right):
    return lax.dot_general(
        left, right, (((1,), (1,)), ((), ())), preferred_element_type=jnp.float32
    )


def fold(product, rows, columns):
    upper = product[:rows, :columns] + product[rows:, :columns]
    lower = product[:rows, columns:] + product[rows:, columns:]
    return upper + lower


def kernel(
    row_count, group, chunks, width,
    a_ref, tile_ref, b_ref, ids_ref,
    sol_ref, res_ref,
    a_buf, a_split, tile_split, v_split, u_buf, m_buf,
    part, near, half, far, full, image,
    dot_own, dot_in, sums, i_buf, ids_buf,
    a_sem, near_sem, far_sem, full_sem, line_recv, line_send, side_recv, side_send, dot_send, dot_recv,
):
    my_row, my_col = lax.axis_index("row"), lax.axis_index("col")
    depth = row_count // group
    place, lane = my_row // group, lax.rem(my_row, group)
    core = lax.rem(my_col, 2)
    partner = my_col + 1 - 2 * core
    across = lax.rem(my_col + 2, 4)
    nrhs, block_cols = b_ref.shape
    block_rows = a_ref.shape[0]
    hh = nrhs // 2
    tiles = block_cols // width
    steps = block_rows // width
    piece = block_rows // chunks

    def fetch(i):
        rows = pl.ds(pl.multiple_of(i * width, width), width)
        return pltpu.make_async_copy(a_ref.at[rows], a_buf.at[i], a_sem.at[i])

    @pl.loop(0, steps)
    def _(i):
        fetch(i).start()

    barrier = pltpu.get_barrier_semaphore()
    for shift in range(1, 4):
        pl.semaphore_signal(
            barrier, inc=1, device_id=(my_row, lax.rem(my_col + shift, 4)), device_id_type=MESH
        )
    for shift in range(1, group):
        side = place * group + lax.rem(lane + shift, group)
        pl.semaphore_signal(barrier, inc=1, device_id=(side, my_col), device_id_type=MESH)

    @pl.when(place > 0)
    def _():
        pl.semaphore_signal(barrier, inc=1, device_id=(my_row - group, my_col), device_id_type=MESH)

    @pl.when(place < depth - 1)
    def _():
        pl.semaphore_signal(barrier, inc=1, device_id=(my_row + group, my_col), device_id_type=MESH)

    def tile_lanes(t):
        return pl.ds(pl.multiple_of(t * width, width), width)

    def precondition_tile(t, value, target):
        lanes = tile_lanes(t)
        value = fold(times_transposed(split(value), tile_split[t]), nrhs, width)
        target[:, lanes] = value
        v_split[:, lanes] = split(value)

    ids_buf[...] = jnp.zeros_like(ids_buf)
    ids_buf[0:tiles] = ids_ref[...].astype(jnp.float32)
    ids_across = ids_buf[...].T
    for t in range(tiles):
        same = ids_across[:, t : t + 1] == ids_buf[t : t + 1]
        tile_split[t] = split(jnp.where(same, tile_ref[t], 0.0))

    @pl.loop(0, tiles)
    def _(t):
        precondition_tile(t, b_ref[:, tile_lanes(t)], u_buf)

    mine = pl.ds(pl.multiple_of(core * hh, hh), hh)
    other = pl.ds(pl.multiple_of((1 - core) * hh, hh), hh)
    goes_up = jnp.logical_and(place >= my_col, place < depth - 1)
    goes_down = jnp.logical_and(place <= my_col, place > 0)
    per_chunk = steps // chunks

    def multiply_and_spread(turn, make, use):
        def swap(source, target, sem, column, q):
            return pltpu.make_async_remote_copy(
                src_ref=source, dst_ref=target, send_sem=sem.at[turn, 0, q], recv_sem=sem.at[turn, 1, q],
                device_id=(my_row, column), device_id_type=MESH,
            )

        def cut(q):
            return pl.ds(q * piece, piece)

        def first(q):
            return swap(part.at[turn, other, cut(q)], near.at[turn, :, cut(q)], near_sem, partner, q)

        def second(q):
            return swap(half.at[turn, :, cut(q)], far.at[turn, :, cut(q)], far_sem, across, q)

        def third(q):
            return swap(full.at[turn, mine, cut(q)], full.at[turn, mine, cut(q)], full_sem, partner, q)

        def lanes_of(owner, q):
            return pl.ds(pl.multiple_of(owner * block_rows + q * piece, width), piece)

        def along(q, way, target_row):
            return pltpu.make_async_remote_copy(
                src_ref=image.at[turn, :, lanes_of(lane, q)], dst_ref=image.at[turn, :, lanes_of(lane, q)],
                send_sem=line_send.at[turn, way, q], recv_sem=line_recv.at[turn, q],
                device_id=(target_row, my_col), device_id_type=MESH,
            )

        def sideways(q, shift, owner, side):
            return pltpu.make_async_remote_copy(
                src_ref=image.at[turn, :, lanes_of(owner, q)], dst_ref=image.at[turn, :, lanes_of(owner, q)],
                send_sem=side_send.at[turn, shift - 1, q], recv_sem=side_recv.at[turn, shift - 1, q],
                device_id=(side, my_col), device_id_type=MESH,
            )

        def outgoing(q, shift):
            return sideways(q, shift, lane, place * group + lax.rem(lane + shift, group))

        def pass_on(q):
            @pl.when(goes_up)
            def _():
                along(q, 0, my_row + group).start()

            @pl.when(goes_down)
            def _():
                along(q, 1, my_row - group).start()

            for shift in range(1, group):
                outgoing(q, shift).start()

        def stage0(q):
            @pl.loop(q * per_chunk, (q + 1) * per_chunk)
            def _(i):
                part[turn, :, tile_lanes(i)] = make(i)

            if turn == 0 and q == 0:
                pl.semaphore_wait(
                    barrier,
                    3 + (group - 1) + jnp.where(place > 0, 1, 0) + jnp.where(place < depth - 1, 1, 0),
                )
            first(q).start()

        def stage1(q):
            first(q).wait()
            half[turn, :, cut(q)] = part[turn, mine, cut(q)] + near[turn, :, cut(q)]
            second(q).start()

        def stage2(q):
            second(q).wait()
            full[turn, mine, cut(q)] = half[turn, :, cut(q)] + far[turn, :, cut(q)]
            third(q).start()

        def stage3(q):
            third(q).wait()

            @pl.when(place == my_col)
            def _():
                image[turn, :, lanes_of(lane, q)] = full[turn, :, cut(q)]
                pass_on(q)

        for tick in range(chunks + LAGS[-1]):
            for lag, stage in zip(LAGS, (stage0, stage1, stage2, stage3)):
                if 0 <= tick - lag < chunks:
                    stage(tick - lag)

        @pl.when(place != my_col)
        def _():
            for q in range(chunks):
                along(q, 0, my_row).wait_recv()
                pass_on(q)

        if turn == 1:
            for shift in range(1, 4):
                dots_copy(0, shift).wait()
        for q in range(chunks):
            use(lane * steps + q * per_chunk, per_chunk)
        for q in range(chunks):
            for shift in range(1, group):
                origin = lax.rem(lane + group - shift, group)
                sideways(q, shift, origin, place * group + origin).wait_recv()
                use(origin * steps + q * per_chunk, per_chunk)

        def finish():
            for q in range(chunks):
                @pl.when(goes_up)
                def _():
                    along(q, 0, my_row + group).wait_send()

                @pl.when(goes_down)
                def _():
                    along(q, 1, my_row - group).wait_send()

                for shift in range(1, group):
                    outgoing(q, shift).wait_send()

        return finish

    def dots_copy(turn, shift):
        return pltpu.make_async_remote_copy(
            src_ref=dot_own.at[turn], dst_ref=dot_in.at[turn, shift - 1],
            send_sem=dot_send.at[turn, shift - 1], recv_sem=dot_recv.at[turn, shift - 1],
            device_id=(my_row, lax.rem(my_col + shift, 4)), device_id_type=MESH,
        )

    def pack(gamma, delta):
        place_of = lax.broadcasted_iota(jnp.int32, (nrhs, width), 1)
        gamma = jnp.sum(gamma, axis=1, keepdims=True)
        delta = jnp.sum(delta, axis=1, keepdims=True)
        return jnp.where(place_of == 0, gamma, jnp.where(place_of == 1, delta, 0.0))

    def unpack(turn):
        total = [dot_own[turn]] + [dot_in[turn, (3 - my_col_shift)] for my_col_shift in (1, 2, 3)]
        total = (total[0] + total[2]) + (total[1] + total[3])
        return total[:, 0:1], total[:, 1:2]

    sums[...] = jnp.zeros_like(sums)

    def first_product(i):
        fetch(i).wait()
        parts = split(a_buf[i])
        a_split[i] = parts
        return fold(times_transposed(v_split[...], parts), nrhs, width)

    def second_product(i):
        return fold(times_transposed(v_split[...], a_split[i]), nrhs, width)

    def first_use(begin, count):
        @pl.loop(begin, begin + count)
        def _(t):
            lanes = tile_lanes(t)
            u, w = u_buf[:, lanes], image[0, :, lanes]
            sums[0] += b_ref[:, lanes] * u
            sums[1] += w * u
            precondition_tile(t, w, m_buf)

    finish_first = multiply_and_spread(0, first_product, first_use)
    dot_own[0] = pack(sums[0], sums[1])
    for shift in (2, 1, 3):
        dots_copy(0, shift).start()
    sums[...] = jnp.zeros_like(sums)

    def second_use(begin, count):
        gamma0, delta0 = unpack(0)
        alpha0 = gamma0 / delta0

        @pl.loop(begin, begin + count)
        def _(t):
            lanes = tile_lanes(t)
            w, u = image[0, :, lanes], u_buf[:, lanes]
            res = b_ref[:, lanes] - alpha0 * w
            pre = u - alpha0 * m_buf[:, lanes]
            img = w - alpha0 * image[1, :, lanes]
            res_ref[:, lanes] = res
            sol_ref[:, lanes] = alpha0 * u
            m_buf[:, lanes] = pre
            i_buf[:, lanes] = img
            sums[0] += res * pre
            sums[1] += img * pre

    finish_second = multiply_and_spread(1, second_product, second_use)
    dot_own[1] = pack(sums[0], sums[1])
    for shift in (2, 1, 3):
        dots_copy(1, shift).start()
    finish_first()
    finish_second()
    for shift in range(1, 4):
        dots_copy(1, shift).wait()
    gamma0, delta0 = unpack(0)
    alpha0 = gamma0 / delta0
    gamma1, delta1 = unpack(1)
    beta = gamma1 / gamma0
    alpha1 = gamma1 / (delta1 - beta * gamma1 / alpha0)

    @pl.loop(0, tiles)
    def _(t):
        lanes = tile_lanes(t)
        sol_ref[:, lanes] += alpha1 * (m_buf[:, lanes] + beta * u_buf[:, lanes])
        res_ref[:, lanes] -= alpha1 * (i_buf[:, lanes] + beta * image[0, :, lanes])


def fused_body(row_count, group, normal_matrix, right_side, tile_inverse, order_ids):
    block_rows, block_cols = normal_matrix.shape
    nrhs = right_side.shape[1]
    tiles, width = tile_inverse.shape[:2]
    steps = block_rows // width
    chunks = CHUNKS if steps % CHUNKS == 0 else 1
    f32, bf16 = jnp.float32, jnp.bfloat16
    out = jax.ShapeDtypeStruct((nrhs, block_cols), f32)
    dma = pltpu.SemaphoreType.DMA
    vmem = pl.BlockSpec(memory_space=pltpu.VMEM)
    sol, res = pl.pallas_call(
        functools.partial(kernel, row_count, group, chunks, width),
        out_shape=(out, out),
        in_specs=[pl.BlockSpec(memory_space=pl.ANY), vmem, vmem, vmem],
        out_specs=(vmem, vmem),
        scratch_shapes=[
            pltpu.VMEM((steps, width, block_cols), f32),
            pltpu.VMEM((steps, 2 * width, block_cols), bf16),
            pltpu.VMEM((tiles, 2 * width, width), bf16),
            pltpu.VMEM((2 * nrhs, block_cols), bf16),
            pltpu.VMEM((nrhs, block_cols), f32),
            pltpu.VMEM((nrhs, block_cols), f32),
            pltpu.VMEM((2, nrhs, block_rows), f32),
            pltpu.VMEM((2, nrhs // 2, block_rows), f32),
            pltpu.VMEM((2, nrhs // 2, block_rows), f32),
            pltpu.VMEM((2, nrhs // 2, block_rows), f32),
            pltpu.VMEM((2, nrhs, block_rows), f32),
            pltpu.VMEM((2, nrhs, block_cols), f32),
            pltpu.VMEM((2, nrhs, width), f32),
            pltpu.VMEM((2, 3, nrhs, width), f32),
            pltpu.VMEM((2, nrhs, width), f32),
            pltpu.VMEM((nrhs, block_cols), f32),
            pltpu.VMEM((width, width), f32),
            dma((steps,)),
            dma((2, 2, chunks)),
            dma((2, 2, chunks)),
            dma((2, 2, chunks)),
            dma((2, chunks)),
            dma((2, 2, chunks)),
            dma((2, group - 1, chunks)),
            dma((2, group - 1, chunks)),
            dma((2, 3)),
            dma((2, 3)),
        ],
        compiler_params=pltpu.CompilerParams(
            collective_id=0, has_side_effects=True, vmem_limit_bytes=60 * 1024 * 1024
        ),
    )(normal_matrix, tile_inverse, right_side.T, order_ids.reshape(tiles, width))
    return sol.T, res.T


def body(row_count, col_count, normal_matrix, right_side, tile_inverse, order_ids):
    block_rows, block_cols = normal_matrix.shape
    width = tile_inverse.shape[1]
    group = block_cols // block_rows
    fits = (
        col_count == 4
        and group > 1
        and row_count == group * col_count
        and block_rows % width == 0
        and width % 128 == 0
        and tile_inverse.shape[0] <= width
        and right_side.shape[1] % 32 == 0
    )
    if fits:
        return fused_body(row_count, group, normal_matrix, right_side, tile_inverse, order_ids)
    return plain_body(normal_matrix, right_side, tile_inverse, order_ids)


def solution(mesh):
    return jax.shard_map(
        functools.partial(body, mesh.shape["row"], mesh.shape["col"]),
        mesh=mesh,
        in_specs=(P("row", "col"), P("col", None), P("col", None, None), P("col")),
        out_specs=(P("col", None), P("col", None)),
        check_vma=False,
    )
```
